8 devices in a mesh: dp: 1 (over z), sp: 8 (over x, y, core).
Axes of the slice: x: 2, y: 2, z: 1, core: 2. Of those that a mesh axis runs over, the one named last changes fastest.
Arguments:
- x: bfloat16 [1024, 4096], P(('dp', 'sp'))
- gain: bfloat16 [4096], replicated
- wq: bfloat16 [4096, 4096], replicated
- wk: bfloat16 [4096, 256], replicated
- wv: bfloat16 [4096, 256], replicated
- wo: bfloat16 [4096, 4096], replicated
Outputs:
- output: bfloat16 [1024, 4096], P(('dp', 'sp'))
All inputs are finite; a program needn't handle non-finite values.
Results may differ from the reference program's by a relative error of at most 0.012.
Values are sent between devices in bfloat16 or wider.
A program may use at most 2 GiB of HBM per device.

```python
import jax
import jax.numpy as jnp
from jax import lax

ROWS = 1024
D = 4096
HEADS = 16
KV_HEADS = 1
HEAD = 256
THETA = 10000


def setup_inputs(seed: int = 0, part: int = 0) -> dict:
    kx, kn, kq, kk, kv, ko = jax.random.split(jax.random.key(seed), 6)

    def weights(key, rows, columns):
        return jax.random.normal(key, (rows, columns), jnp.float32) * rows**-0.5

    drawn = {
        "x": jax.random.normal(jax.random.fold_in(kx, part), (ROWS, D), jnp.float32),
        "gain": 1 + 0.1 * jax.random.normal(kn, (D,), jnp.float32),
        "wq": 2 * weights(kq, D, HEADS * HEAD),
        "wk": 2 * weights(kk, D, KV_HEADS * HEAD),
        "wv": 4 * weights(kv, D, KV_HEADS * HEAD),
        "wo": weights(ko, HEADS * HEAD, D),
    }
    return {k: v.astype(jnp.bfloat16) for k, v in drawn.items()}


def normed(x, gain):
    wide = x.astype(jnp.float32)
    scale = lax.rsqrt(jnp.mean(wide * wide, -1, keepdims=True) + 1e-6)
    return (wide * scale * gain.astype(jnp.float32)).astype(jnp.bfloat16)


def turned(t, place, theta):
    half = t.shape[-1] // 2
    angle = place.astype(jnp.float32)[:, None] * theta ** (-jnp.arange(half, dtype=jnp.float32) / half)
    cos, sin = jnp.cos(angle)[:, None], jnp.sin(angle)[:, None]
    a, b = t[..., :half].astype(jnp.float32), t[..., half:].astype(jnp.float32)
    return jnp.concatenate([a * cos - b * sin, b * cos + a * sin], -1).astype(jnp.bfloat16)


def matmul(a, w):
    return jnp.dot(a, w, preferred_element_type=jnp.float32).astype(jnp.bfloat16)


def einsum(form, a, b):
    return jnp.einsum(form, a.astype(jnp.float32), b.astype(jnp.float32))


def attention(q, k, v):
    scores = einsum("tgsd,ugd->gstu", q, k) * q.shape[-1] ** -0.5
    token = jnp.arange(q.shape[0])
    scores = jnp.where(token[:, None] >= token, scores, -jnp.inf)
    weights = jax.nn.softmax(scores, -1).astype(jnp.bfloat16)
    return einsum("gstu,ugd->tgsd", weights, v).astype(jnp.bfloat16)


def reference(x, gain, wq, wk, wv, wo):
    a, place = normed(x, gain), jnp.arange(ROWS)
    q = turned(matmul(a, wq).reshape(ROWS, HEADS, HEAD), place, THETA).reshape(ROWS, KV_HEADS, -1, HEAD)
    k = turned(matmul(a, wk).reshape(ROWS, KV_HEADS, HEAD), place, THETA)
    v = matmul(a, wv).reshape(ROWS, KV_HEADS, HEAD)
    seen = attention(q, k, v).reshape(ROWS, HEADS * HEAD)
    return (x.astype(jnp.float32) + jnp.dot(seen, wo, preferred_element_type=jnp.float32)).astype(jnp.bfloat16)
```

```python
import functools

import jax
import jax.numpy as jnp
import numpy as np
from jax import lax
from jax.experimental import pallas as pl
from jax.experimental.pallas import tpu as pltpu
from jax.sharding import PartitionSpec as P

HEAD = 256
THETA = 10000
LOG2E = 1.4426950408889634
VMEM = 63 * 2**20
MESH = pl.DeviceIdType.MESH
OWN = 128
PAIR = 256
D = 4096
HALF = D // 2
CHIPS = 4
NQ = 4
NO = 8
QW, OW = HALF // NQ, HALF // NO


def _dot(a, b):
    return jnp.dot(a, b, preferred_element_type=jnp.float32)


def _kernel(x_hbm, gain_hbm, wq_hbm, wk_hbm, wv_hbm, wo_hbm, cos_hbm, sin_hbm, out,
            xs, gv, cs, sn, a, wkv, wvv, wqv, wov, kt, vv, qv, seen, ysend,
            xsem, tsem, wsem, qsem, osem, xr, kr, vr, sr, yr, xsend, ks, vs, fs, ss, ys):
    me = lax.axis_index("sp")
    core = lax.rem(me, 2)
    chip = lax.div(me, 2)
    other = me + 1 - 2 * core
    mine = pl.ds(pl.multiple_of(core * OWN, OWN), OWN)
    theirs = pl.ds(pl.multiple_of(OWN - core * OWN, OWN), OWN)

    def block(i):
        return pl.ds(pl.multiple_of(i * OWN, OWN), OWN)

    local = []

    def fetch(src, dst, sem):
        c = pltpu.make_async_copy(src, dst, sem)
        c.start()
        return c

    cx = fetch(x_hbm, xs.at[mine, :], xsem)
    ct = [fetch(gain_hbm, gv, tsem.at[0])]
    ck = fetch(wk_hbm, wkv, wsem.at[0])
    cv = fetch(wv_hbm, wvv, wsem.at[1])
    rows = pl.ds(pl.multiple_of(chip * PAIR, PAIR), PAIR)
    ct += [fetch(cos_hbm.at[rows, :], cs, tsem.at[1]), fetch(sin_hbm.at[rows, :], sn, tsem.at[2])]
    cq = [fetch(wq_hbm.at[:, pl.ds(pl.multiple_of(core * HALF + n * QW, QW), QW)], wqv.at[n], qsem.at[n]) for n in range(NQ)]
    co = []
    for n in range(NO):
        cols = pl.ds(pl.multiple_of(core * HALF + n * OW, OW), OW)
        co.append([fetch(wo_hbm.at[pl.ds(pl.multiple_of(core * HALF, HALF), HALF), cols], wov.at[n, :HALF, :], osem.at[n, 0]),
                   fetch(wo_hbm.at[pl.ds(pl.multiple_of(HALF - core * HALF, HALF), HALF), cols], wov.at[n, HALF:, :], osem.at[n, 1])])

    barrier = pltpu.get_barrier_semaphore()
    pl.semaphore_signal(barrier, inc=1, device_id={"sp": other}, device_id_type=MESH)
    for step in range(1, CHIPS):
        peer = lax.rem(chip + step, CHIPS) * 2 + core
        pl.semaphore_signal(barrier, inc=1, device_id={"sp": peer}, device_id_type=MESH)
    pl.semaphore_wait(barrier, CHIPS)

    def remote(src, dst, send, recv, to):
        return pltpu.make_async_remote_copy(src_ref=src, dst_ref=dst, send_sem=send, recv_sem=recv, device_id={"sp": to}, device_id_type=MESH)

    cx.wait()
    sx = remote(xs.at[mine, :], xs.at[mine, :], xsend, xr, other)
    sx.start()
    for c in ct:
        c.wait()

    def norm(start):
        @pl.loop(0, OWN // 16)
        def _(i):
            at = pl.ds(pl.multiple_of(start + i * 16, 16), 16)
            wide = xs[at, :].astype(jnp.float32)
            scale = lax.rsqrt(jnp.mean(wide * wide, -1, keepdims=True) + 1e-6)
            a[at, :] = (wide * scale * gv[...].astype(jnp.float32)).astype(jnp.bfloat16)

    def turn(t, cos, sin):
        t = t.astype(jnp.bfloat16).astype(jnp.float32)
        p, q = t[:, :128], t[:, 128:]
        return jnp.concatenate([p * cos - q * sin, q * cos + p * sin], -1).astype(jnp.bfloat16)

    norm(core * OWN)
    ck.wait()
    k = turn(_dot(a[mine, :], wkv[...]), cs[mine, :], sn[mine, :])
    kt[:, block(me)] = k.T

    def send(buf, at, sems, recvs):
        remote(at(buf), at(buf), sems.at[0], recvs.at[me], other).start()
        for c in range(1, CHIPS):
            @pl.when(chip < c)
            def _():
                remote(at(buf), at(buf), sems.at[c], recvs.at[me], c * 2 + core).start()

    send(kt, lambda b: b.at[:, block(me)], ks, kr)
    cv.wait()
    vv[block(me), :] = _dot(a[mine, :], wvv[...]).astype(jnp.bfloat16)
    send(vv, lambda b: b.at[block(me), :], vs, vr)

    sx_in = remote(xs.at[theirs, :], xs.at[theirs, :], xsend, xr, other)
    sx_in.wait_recv()
    norm(OWN - core * OWN)

    for n in range(NQ):
        cq[n].wait()
        for i in range(QW // HEAD):
            qv[n * (QW // HEAD) + i] = turn(_dot(a[...], wqv[n, :, i * HEAD:(i + 1) * HEAD]), cs[...], sn[...])

    def kcopy(i, sem):
        return remote(kt.at[:, block(i)], kt.at[:, block(i)], sem, kr.at[i], other)

    def vcopy(i, sem):
        return remote(vv.at[block(i), :], vv.at[block(i), :], sem, vr.at[i], other)

    for c in range(CHIPS - 1):
        @pl.when(chip > c)
        def _():
            i = c * 2 + core
            kcopy(i, fs.at[0, c]).wait_recv()
            kcopy(i, fs.at[0, c]).start()
            vcopy(i, fs.at[1, c]).wait_recv()
            vcopy(i, fs.at[1, c]).start()
    kcopy(other, ks.at[0]).wait_recv()
    vcopy(other, vs.at[0]).wait_recv()
    for c in range(CHIPS - 1):
        @pl.when(chip > c)
        def _():
            i = c * 2 + 1 - core
            kcopy(i, fs.at[0, c]).wait_recv()
            vcopy(i, fs.at[1, c]).wait_recv()

    e = HEAD ** -0.5 * LOG2E
    keep = lax.broadcasted_iota(jnp.int32, (PAIR, PAIR), 0) >= lax.broadcasted_iota(jnp.int32, (PAIR, PAIR), 1)
    for c in range(CHIPS):
        @pl.when(chip == c)
        def _():
            @pl.loop(0, 8)
            def _(h):
                q = qv[h]
                s = [_dot(q, kt[:, j * PAIR:(j + 1) * PAIR]) for j in range(c + 1)]
                s[c] = jnp.where(keep, s[c], -1e30)
                top = functools.reduce(jnp.maximum, [t.max(-1, keepdims=True) for t in s])
                p = [jnp.exp2((t - top) * e) for t in s]
                total = functools.reduce(jnp.add, [t.sum(-1, keepdims=True) for t in p])
                o = functools.reduce(jnp.add, [_dot(t.astype(jnp.bfloat16), vv[j * PAIR:(j + 1) * PAIR, :]) for j, t in enumerate(p)])
                cols = pl.ds(pl.multiple_of(h * HEAD, HEAD), HEAD)
                seen[:, cols] = (o * (1 / total)).astype(jnp.bfloat16)
                remote(seen.at[:, cols], seen.at[:, pl.ds(pl.multiple_of(HALF + h * HEAD, HEAD), HEAD)], ss.at[h], sr.at[h], other).start()

    def scopy(h):
        return remote(seen.at[:, h * HEAD:(h + 1) * HEAD], seen.at[:, HALF + h * HEAD:HALF + (h + 1) * HEAD], ss.at[h], sr.at[h], other)

    for h in range(8):
        scopy(h).wait_recv()

    def ycopy(n):
        cols = pl.ds(pl.multiple_of(core * HALF + n * OW, OW), OW)
        return remote(ysend.at[:, n * OW:(n + 1) * OW], out.at[:, cols], ys.at[n], yr.at[n], other)

    for n in range(NO):
        for c in co[n]:
            c.wait()
        cols = pl.ds(pl.multiple_of(core * HALF + n * OW, OW), OW)
        y = _dot(seen[...], wov[n]) + xs[:, cols].astype(jnp.float32)
        y = y.astype(jnp.bfloat16)

        @pl.when(core == 0)
        def _():
            out[:, n * OW:(n + 1) * OW] = y[:OWN]
            ysend[:, n * OW:(n + 1) * OW] = y[OWN:]

        @pl.when(core == 1)
        def _():
            out[:, HALF + n * OW:HALF + (n + 1) * OW] = y[OWN:]
            ysend[:, n * OW:(n + 1) * OW] = y[:OWN]
        ycopy(n).start()

    for n in range(NO):
        ycopy(n).wait()
    for h in range(8):
        scopy(h).wait_send()
    sx.wait_send()
    kcopy(me, ks.at[0]).wait_send()
    vcopy(me, vs.at[0]).wait_send()
    for c in range(1, CHIPS):
        @pl.when(chip < c)
        def _():
            kcopy(me, ks.at[c]).wait_send()
            vcopy(me, vs.at[c]).wait_send()
    for c in range(CHIPS - 1):
        @pl.when(chip > c)
        def _():
            kcopy(c * 2 + core, fs.at[0, c]).wait_send()
            vcopy(c * 2 + core, fs.at[1, c]).wait_send()


def _tables():
    half = HEAD // 2
    rate = np.float32(THETA) ** (-np.arange(half, dtype=np.float32) / np.float32(half))
    angle = np.arange(1024, dtype=np.float32)[:, None] * rate.astype(np.float32)
    return np.cos(angle).astype(np.float32), np.sin(angle).astype(np.float32)


def solution(mesh):
    def step(x, gain, wq, wk, wv, wo):
        cos, sin = (jnp.asarray(t) for t in _tables())
        bf, dma = jnp.bfloat16, pltpu.SemaphoreType.DMA
        return pl.pallas_call(
            _kernel,
            out_shape=jax.ShapeDtypeStruct((OWN, D), bf),
            in_specs=[pl.BlockSpec(memory_space=pl.ANY)] * 8,
            out_specs=pl.BlockSpec(memory_space=pltpu.VMEM),
            scratch_shapes=[
                pltpu.VMEM((PAIR, D), bf),
                pltpu.VMEM((1, D), bf),
                pltpu.VMEM((PAIR, 128), jnp.float32), pltpu.VMEM((PAIR, 128), jnp.float32),
                pltpu.VMEM((PAIR, D), bf),
                pltpu.VMEM((D, HEAD), bf), pltpu.VMEM((D, HEAD), bf),
                pltpu.VMEM((NQ, D, QW), bf),
                pltpu.VMEM((NO, D, OW), bf),
                pltpu.VMEM((HEAD, 1024), bf), pltpu.VMEM((1024, HEAD), bf),
                pltpu.VMEM((8, PAIR, HEAD), bf),
                pltpu.VMEM((PAIR, D), bf),
                pltpu.VMEM((OWN, HALF), bf),
                dma, dma((3,)), dma((2,)), dma((NQ,)), dma((NO, 2)),
                dma, dma((8,)), dma((8,)), dma((8,)), dma((NO,)),
                dma, dma((4,)), dma((4,)), dma((2, 4)), dma((8,)), dma((NO,)),
            ],
            compiler_params=pltpu.CompilerParams(collective_id=0, has_side_effects=True, vmem_limit_bytes=VMEM),
        )(x, gain.reshape(1, D), wq, wk, wv, wo, cos, sin)

    tokens, whole = P(("dp", "sp"), None), P(None, None)
    return jax.shard_map(
        step,
        mesh=mesh,
        in_specs=(tokens, P(None), whole, whole, whole, whole),
        out_specs=tokens,
        check_vma=False,
    )
```

```python
import functools

import jax
import jax.numpy as jnp
import numpy as np
from jax import lax
from jax.experimental import pallas as pl
from jax.experimental.pallas import tpu as pltpu
from jax.sharding import PartitionSpec as P

HEAD = 256
THETA = 10000
LOG2E = 1.4426950408889634
VMEM = 60 * 2**20
MESH = pl.DeviceIdType.MESH
OWN = 128
PAIR = 256
D = 4096
HALF = D // 2
CHIPS = 4
NQ = 4
NO = 2
QW, OW = HALF // NQ, HALF // NO
XR = 32
HOPS = ((0, 2), (1, 3), (2, 3)), ((0, 1), (1, 2)), ((0, 3),)
EARLY = (), (0,), (0,), (1,)
LATE = (), (), (1,), (2, 0)
AFTER = 3, 5
SG = 2


def _dot(a, b):
    return jnp.dot(a, b, preferred_element_type=jnp.float32)


def _kernel(x_hbm, gain_hbm, wq_hbm, wk_hbm, wv_hbm, wo_hbm, cos_hbm, sin_hbm, out,
            xo, xp, gv, cs, sn, a, wkv, wqv, wov, kv, qv, seen, y, stat, ysend, ready,
            xsem, tsem, wsem, qsem, osem, xr, kr, sr, yr, xsend, ks, fs, ss, ys):
    me = lax.axis_index("sp")
    core = lax.rem(me, 2)
    chip = lax.div(me, 2)
    other = me + 1 - 2 * core
    mine = pl.ds(pl.multiple_of(core * OWN, OWN), OWN)
    theirs = pl.ds(pl.multiple_of(OWN - core * OWN, OWN), OWN)
    scope = jax.named_scope

    def block(i):
        return pl.ds(pl.multiple_of(i * OWN, OWN), OWN)

    def fetch(src, dst, sem):
        c = pltpu.make_async_copy(src, dst, sem)
        c.start()
        return c

    def qfetch(n):
        return fetch(wq_hbm.at[:, pl.ds(pl.multiple_of(core * HALF + n * QW, QW), QW)], wqv.at[n], qsem.at[n])

    def ofetch(n):
        cols = pl.ds(pl.multiple_of(core * HALF + n * OW, OW), OW)
        return [fetch(wo_hbm.at[pl.ds(pl.multiple_of(core * HALF, HALF), HALF), cols], wov.at[n, :HALF, :], osem.at[n, 0]),
                fetch(wo_hbm.at[pl.ds(pl.multiple_of(HALF - core * HALF, HALF), HALF), cols], wov.at[n, HALF:, :], osem.at[n, 1])]

    cx = fetch(x_hbm, xo, xsem)
    cg = fetch(gain_hbm, gv, tsem.at[0])
    barrier = pltpu.get_barrier_semaphore()
    pl.semaphore_signal(barrier, inc=1, device_id={"sp": other}, device_id_type=MESH)
    for c in range(1, CHIPS):
        @pl.when(chip < c)
        def _():
            pl.semaphore_signal(barrier, inc=1, device_id={"sp": c * 2 + core}, device_id_type=MESH)
    ck = [fetch(wk_hbm, wkv.at[:, :HEAD], wsem.at[0]), fetch(wv_hbm, wkv.at[:, HEAD:], wsem.at[1])]
    rows = pl.ds(pl.multiple_of(chip * PAIR, PAIR), PAIR)
    ct = [fetch(cos_hbm.at[rows, :], cs, tsem.at[1]), fetch(sin_hbm.at[rows, :], sn, tsem.at[2])]
    with scope("barrier"):
        pl.semaphore_wait(barrier, 1 + chip)
    for c in range(CHIPS - 1):
        @pl.when(chip > c)
        def _():
            pl.semaphore_signal(ready.at[chip], inc=1, device_id={"sp": c * 2 + core}, device_id_type=MESH)

    def remote(src, dst, send, recv, to):
        return pltpu.make_async_remote_copy(src_ref=src, dst_ref=dst, send_sem=send, recv_sem=recv, device_id={"sp": to}, device_id_type=MESH)

    def xcopy(i):
        return remote(xo.at[i * XR:(i + 1) * XR, :], xp.at[i * XR:(i + 1) * XR, :], xsend.at[i], xr.at[i], other)

    with scope("x_wait"):
        cx.wait()
    cq = [qfetch(n) for n in range(NQ)]
    co = []
    for i in range(OWN // XR):
        xcopy(i).start()
    with scope("g_wait"):
        cg.wait()

    def norm(src, start):
        for i in range(OWN // 16):
            at = pl.ds(pl.multiple_of(start + i * 16, 16), 16)
            wide = src[i * 16:(i + 1) * 16, :].astype(jnp.float32)
            scale = lax.rsqrt(jnp.mean(wide * wide, -1, keepdims=True) + 1e-6)
            a[at, :] = (wide * scale * gv[...].astype(jnp.float32).reshape(1, D)).astype(jnp.bfloat16)

    def turn(t, cos, sin):
        t = t.astype(jnp.bfloat16).astype(jnp.float32)
        p, q = t[:, :128], t[:, 128:]
        return jnp.concatenate([p * cos - q * sin, q * cos + p * sin], -1).astype(jnp.bfloat16)

    with scope("norm_own"):
        norm(xo, core * OWN)
    with scope("kv_wait"):
        for c in ck + ct:
            c.wait()
    with scope("kv_proj"):
        t = _dot(a[mine, :], wkv[...])
        v = t[:, HEAD:].astype(jnp.bfloat16)
        kv[me, :HEAD, :] = turn(t[:, :HEAD], cs[mine, :], sn[mine, :]).T
        kv[me, HEAD:HEAD + OWN, :] = v[:, :128]
        kv[me, HEAD + OWN:, :] = v[:, 128:]

    def kcopy(i, sem, to):
        return remote(kv.at[i], kv.at[i], sem, kr.at[i], to)

    kcopy(me, ks.at[0], other).start()
    for hop in (1, 2, 3):
        for c, to in HOPS[hop - 1]:
            @pl.when(chip == c)
            @scope("ready")
            def _():
                pl.semaphore_wait(ready.at[to], 1)
                kcopy(me, ks.at[to], to * 2 + core).start()

    def arrived(c, mine):
        kcopy(c * 2 + (core if mine else 1 - core), fs.at[c], other).wait_recv()

    def forward(c):
        arrived(c, True)
        kcopy(c * 2 + core, fs.at[c], other).start()

    with scope("xother_wait"):
        for i in range(OWN // XR):
            xcopy(i).wait_recv()
    with scope("q_wait"):
        cq[0].wait()

    def queries(n, at):
        t = _dot(a[at, :], wqv[n])
        for i in range(QW // HEAD):
            qv[n * (QW // HEAD) + i, at, :] = turn(t[:, i * HEAD:(i + 1) * HEAD], cs[at, :], sn[at, :])

    with scope("norm_other_q0"):
        queries(0, mine)
        norm(xp, OWN - core * OWN)
    with scope("q0"):
        queries(0, theirs)
    for n in range(2):
        co.append(ofetch(n))
    for n in range(1, NQ):
        with scope("q_wait"):
            cq[n].wait()
        with scope("q_proj"):
            queries(n, slice(None))
        if n == 2:
            with scope("forward"):
                for c in range(1, CHIPS):
                    @pl.when(chip == c)
                    def _():
                        for i in EARLY[c]:
                            forward(i)

    kcopy(other, ks.at[0], other).wait_recv()

    def scopy(g):
        w = HALF // SG
        return remote(seen.at[:, g * w:(g + 1) * w], seen.at[:, HALF + g * w:HALF + (g + 1) * w], ss.at[g], sr.at[g], other)

    e = HEAD ** -0.5 * LOG2E

    def attend(early, late):
        def scores(h, chips):
            return _dot(qv[h], jnp.concatenate([kv[2 * c + i, :HEAD, :] for c in chips for i in (0, 1)], 1))

        def values(chips):
            return jnp.concatenate([jnp.concatenate([kv[2 * c + i, HEAD:HEAD + OWN, :], kv[2 * c + i, HEAD + OWN:, :]], 1)
                                    for c in chips for i in (0, 1)], 0)

        def spread(t):
            return jnp.broadcast_to(t, (PAIR, 128))

        def finish(h, s, chips, first):
            s = [s[:, i:i + 128] for i in range(0, s.shape[1], 128)]
            if first:
                row = lax.broadcasted_iota(jnp.int32, (PAIR, 128), 0)
                col = lax.broadcasted_iota(jnp.int32, (PAIR, 128), 1)
                s[-2:] = [jnp.where(row >= col, s[-2], -1e30), jnp.where(row >= col + 128, s[-1], -1e30)]
            at = slice(h * HEAD, (h + 1) * HEAD)
            top = spread(functools.reduce(jnp.maximum, s).max(-1, keepdims=True) * e)
            if not first:
                before = stat[0, h]
                top = jnp.maximum(top, before)
                keep = jnp.exp2(before - top)
            p = [jnp.exp2(t * e - top) for t in s]
            total = spread(functools.reduce(jnp.add, p).sum(-1, keepdims=True))
            o = _dot(jnp.concatenate(p, 1).astype(jnp.bfloat16), values(chips))
            if not first:
                total += stat[1, h] * keep
                o += y[:, at] * jnp.concatenate([keep, keep], 1)
            if first and late:
                stat[0, h] = top
                stat[1, h] = total
                y[:, at] = o
                return
            share = 1 / total
            seen[:, at] = (o * jnp.concatenate([share, share], 1)).astype(jnp.bfloat16)
            if (h + 1) % (8 // SG) == 0:
                scopy(h // (8 // SG)).start()

        def heads(chips, first):
            s = scores(0, chips)
            for h in range(8):
                ahead = scores(h + 1, chips) if h < 7 else None
                finish(h, s, chips, first)
                s = ahead
                if first and h in AFTER[:len(late)]:
                    with scope("late_forward"):
                        forward(late[AFTER.index(h)])

        with scope("early_wait"):
            for c in early[:-1]:
                arrived(c, False)
        with scope("early"):
            heads(early, True)
        if late:
            with scope("late_wait"):
                for c in late:
                    arrived(c, False)
            with scope("late"):
                heads(late, False)

    for c in range(CHIPS):
        @pl.when(chip == c)
        def _():
            attend(EARLY[c] + (c,), LATE[c])

    def ycopy(n):
        cols = pl.ds(pl.multiple_of(core * HALF + n * OW, OW), OW)
        return remote(ysend.at[:, n * OW:(n + 1) * OW], out.at[:, cols], ys.at[n], yr.at[n], other)

    for n in range(NO):
        with scope("o_wait"):
            for c in co[n]:
                c.wait()
        with scope("o_first"):
            y[:, n * OW:(n + 1) * OW] = _dot(seen[:, :HALF], wov[n, :HALF, :])
    with scope("seen_wait"):
        for g in range(SG):
            scopy(g).wait_recv()
    for n in range(NO):
        at = slice(n * OW, (n + 1) * OW)
        cols = pl.ds(pl.multiple_of(core * HALF + n * OW, OW), OW)

        def second(rows):
            return y[rows, at] + _dot(seen[rows, HALF:], wov[n, HALF:, :])

        def total(t, x):
            return (t + x[:, cols].astype(jnp.float32)).astype(jnp.bfloat16)

        if n < NO - 1:
            with scope("o_second"):
                y[:, at] = second(slice(None))
            with scope("o_out"):
                ysend[:, at] = total(y[theirs, at], xp)
            ycopy(n).start()
            with scope("o_out"):
                out[:, cols] = total(y[mine, at], xo)
        else:
            with scope("o_theirs"):
                ysend[:, at] = total(second(theirs), xp)
            ycopy(n).start()
            with scope("o_mine"):
                out[:, cols] = total(second(mine), xo)

    with scope("y_wait"):
        for n in range(NO):
            ycopy(n).wait()
    with scope("end_wait"):
        for g in range(SG):
            scopy(g).wait_send()
        for i in range(OWN // XR):
            xcopy(i).wait_send()
        kcopy(me, ks.at[0], other).wait_send()
        for c in range(1, CHIPS):
            @pl.when(chip < c)
            def _():
                kcopy(me, ks.at[c], c * 2 + core).wait_send()
        for c in range(CHIPS - 1):
            @pl.when(chip > c)
            def _():
                kcopy(c * 2 + core, fs.at[c], other).wait_send()


def _tables():
    half = HEAD // 2
    rate = np.float32(THETA) ** (-np.arange(half, dtype=np.float32) / np.float32(half))
    angle = np.arange(1024, dtype=np.float32)[:, None] * rate.astype(np.float32)
    return np.cos(angle).astype(np.float32), np.sin(angle).astype(np.float32)


def solution(mesh):
    def step(x, gain, wq, wk, wv, wo):
        cos, sin = (jnp.asarray(t) for t in _tables())
        bf, dma = jnp.bfloat16, pltpu.SemaphoreType.DMA
        return pl.pallas_call(
            _kernel,
            out_shape=pltpu.VMEM((OWN, D), bf),
            in_specs=[pl.BlockSpec(memory_space=pl.ANY)] * 8,
            out_specs=pl.BlockSpec(memory_space=pltpu.VMEM),
            scratch_shapes=[
                pltpu.VMEM((OWN, D), bf), pltpu.VMEM((OWN, D), bf),
                pltpu.VMEM((D,), bf),
                pltpu.VMEM((PAIR, 128), jnp.float32), pltpu.VMEM((PAIR, 128), jnp.float32),
                pltpu.VMEM((PAIR, D), bf),
                pltpu.VMEM((D, 2 * HEAD), bf),
                pltpu.VMEM((NQ, D, QW), bf),
                pltpu.VMEM((NO, D, OW), bf),
                pltpu.VMEM((8, 2 * HEAD, OWN), bf),
                pltpu.VMEM((8, PAIR, HEAD), bf),
                pltpu.VMEM((PAIR, D), bf),
                pltpu.VMEM((PAIR, HALF), jnp.float32),
                pltpu.VMEM((2, 8, PAIR, 128), jnp.float32),
                pltpu.VMEM((OWN, HALF), bf),
                pltpu.SemaphoreType.REGULAR((CHIPS,)),
                dma, dma((3,)), dma((2,)), dma((NQ,)), dma((NO, 2)),
                dma((OWN // XR,)), dma((8,)), dma((SG,)), dma((NO,)),
                dma((OWN // XR,)), dma((4,)), dma((4,)), dma((SG,)), dma((NO,)),
            ],
            compiler_params=pltpu.CompilerParams(collective_id=0, has_side_effects=True, vmem_limit_bytes=VMEM),
        )(x, gain, wq, wk, wv, wo, cos, sin)

    tokens, whole = P(("dp", "sp"), None), P(None, None)
    return jax.shard_map(
        step,
        mesh=mesh,
        in_specs=(tokens, P(None), whole, whole, whole, whole),
        out_specs=tokens,
        check_vma=False,
    )
```

```python
import functools

import jax
import jax.numpy as jnp
import numpy as np
from jax import lax
from jax.experimental import pallas as pl
from jax.experimental.pallas import tpu as pltpu
from jax.sharding import PartitionSpec as P

HEAD = 256
THETA = 10000
LOG2E = 1.4426950408889634
VMEM = 60 * 2**20
MESH = pl.DeviceIdType.MESH
OWN = 128
PAIR = 256
D = 4096
HALF = D // 2
CHIPS = 4
NQ = 4
NO = 2
QW, OW = HALF // NQ, HALF // NO
FIRST = (0, 2), (1, 3), (2, 3), (0, 1)
SECOND = (1, 2),
THIRD = (0, 3),
EARLY = (), (0,), (0,), (1, 2)
LATE = (), (), (1,), (0,)
AFTER = 1,
SG = 2


def _dot(a, b):
    return jnp.dot(a, b, preferred_element_type=jnp.float32)


def _kernel(x_hbm, gain_hbm, wq_hbm, wk_hbm, wv_hbm, wo_hbm, turn_hbm, out,
            xo, xp, gv, cs, a, wkv, wqv, wov, kv, qv, seen, y, stat, ysend, ready,
            lsem, qsem, xr, kr, sr, yr, xsent, ksent, ssent, ysent):
    me = lax.axis_index("sp")
    core = lax.rem(me, 2)
    chip = lax.div(me, 2)
    other = me + 1 - 2 * core
    mine = pl.ds(pl.multiple_of(core * OWN, OWN), OWN)
    theirs = pl.ds(pl.multiple_of(OWN - core * OWN, OWN), OWN)
    scope = jax.named_scope

    def block(i):
        return pl.ds(pl.multiple_of(i * OWN, OWN), OWN)

    def fetch(src, dst, sem):
        c = pltpu.make_async_copy(src, dst, sem)
        c.start()
        return c

    def qfetch(n):
        return fetch(wq_hbm.at[:, pl.ds(pl.multiple_of(core * HALF + n * QW, QW), QW)], wqv.at[n], qsem.at[n])

    def ofetch(n):
        cols = pl.ds(pl.multiple_of(core * HALF + n * OW, OW), OW)
        fetch(wo_hbm.at[pl.ds(pl.multiple_of(core * HALF, HALF), HALF), cols], wov.at[n, :HALF, :], qsem.at[n])
        fetch(wo_hbm.at[pl.ds(pl.multiple_of(HALF - core * HALF, HALF), HALF), cols], wov.at[n, HALF:, :], qsem.at[n])
        return pltpu.make_async_copy(wo_hbm.at[:, cols], wov.at[n], qsem.at[n])

    cx = fetch(x_hbm, xo, lsem.at[0])
    cg = fetch(gain_hbm, gv, lsem.at[1])
    barrier = pltpu.get_barrier_semaphore()
    pl.semaphore_signal(barrier, inc=1, device_id={"sp": other}, device_id_type=MESH)
    for c in range(1, CHIPS):
        @pl.when(chip < c)
        def _():
            pl.semaphore_signal(barrier, inc=1, device_id={"sp": c * 2 + core}, device_id_type=MESH)
    rows = pl.ds(pl.multiple_of(chip * PAIR, PAIR), PAIR)
    ck = [fetch(turn_hbm.at[rows, :], cs, lsem.at[2]), fetch(wk_hbm, wkv.at[:, :HEAD], lsem.at[3])]
    cv = fetch(wv_hbm, wkv.at[:, HEAD:], lsem.at[4])
    with scope("barrier"):
        pl.semaphore_wait(barrier, 1 + chip)
    for c in range(CHIPS - 1):
        @pl.when(chip > c)
        def _():
            pl.semaphore_signal(ready.at[chip], inc=1, device_id={"sp": c * 2 + core}, device_id_type=MESH)

    def remote(src, dst, send, recv, to):
        return pltpu.make_async_remote_copy(src_ref=src, dst_ref=dst, send_sem=send, recv_sem=recv, device_id={"sp": to}, device_id_type=MESH)

    def xcopy():
        return remote(xo, xp, xsent, xr, other)

    with scope("x_wait"):
        cx.wait()
        cg.wait()
    cq = [qfetch(n) for n in range(NQ)]
    xcopy().start()

    def norm(src, start):
        for i in range(OWN // 16):
            at = pl.ds(pl.multiple_of(start + i * 16, 16), 16)
            wide = src[i * 16:(i + 1) * 16, :].astype(jnp.float32)
            scale = lax.rsqrt(jnp.mean(wide * wide, -1, keepdims=True) + 1e-6)
            a[at, :] = (wide * scale * gv[...].astype(jnp.float32).reshape(1, D)).astype(jnp.bfloat16)

    def turn(t, table):
        cos, sin = table[:, :128], table[:, 128:]
        t = t.astype(jnp.bfloat16).astype(jnp.float32)
        p, q = t[:, :128], t[:, 128:]
        return jnp.concatenate([p * cos - q * sin, q * cos + p * sin], -1).astype(jnp.bfloat16)

    with scope("norm_own"):
        norm(xo, core * OWN)
    def kcopy(i, to, part=slice(None)):
        return remote(kv.at[i, part, :], kv.at[i, part, :], ksent, kr.at[i], to)

    def send(pairs, part, wait=False):
        for c, to in pairs:
            @pl.when(chip == c)
            def _():
                if wait:
                    pl.semaphore_wait(ready.at[to], 1)
                kcopy(me, to * 2 + core, part).start()

    keys, values = slice(0, HEAD), slice(HEAD, 2 * HEAD)
    with scope("k_wait"):
        for c in ck:
            c.wait()
    with scope("k_proj"):
        kv[me, :HEAD, :] = turn(_dot(a[mine, :], wkv[:, :HEAD]), cs[mine, :]).T
    kcopy(me, other, keys).start()
    with scope("ready"):
        send([(c, to) for c, to in FIRST if c], keys, True)
    with scope("v_proj"):
        cv.wait()
        v = _dot(a[mine, :], wkv[:, HEAD:]).astype(jnp.bfloat16)
        kv[me, HEAD:HEAD + OWN, :] = v[:, :128]
        kv[me, HEAD + OWN:, :] = v[:, 128:]
    kcopy(me, other, values).start()
    send([(c, to) for c, to in FIRST if c], values)
    send([(c, to) for c, to in FIRST if not c], slice(None), True)

    def arrived(c, mine):
        kcopy(c * 2 + (core if mine else 1 - core), other).wait_recv()

    def forward(c):
        arrived(c, True)
        kcopy(c * 2 + core, other).start()

    with scope("xother_wait"):
        xcopy().wait_recv()
    with scope("q_wait"):
        cq[0].wait()

    def queries(n, at):
        t = _dot(a[at, :], wqv[n])
        for i in range(QW // HEAD):
            qv[n * (QW // HEAD) + i, at, :] = turn(t[:, i * HEAD:(i + 1) * HEAD], cs[at, :])

    with scope("norm_other_q0"):
        queries(0, mine)
        norm(xp, OWN - core * OWN)
    with scope("q0"):
        queries(0, theirs)
    co = [ofetch(0)]
    send(SECOND, slice(None), True)
    for n in range(1, NQ):
        with scope("q_wait"):
            cq[n].wait()
        with scope("q_proj"):
            queries(n, slice(None))
        if n == 1:
            co.append(ofetch(1))
            send(THIRD, slice(None), True)
        if n == 2:
            with scope("forward"):
                for c in range(1, CHIPS):
                    @pl.when(chip == c)
                    def _():
                        for i in EARLY[c]:
                            forward(i)

    kcopy(other, other).wait_recv()

    def scopy(at, w):
        return remote(seen.at[:, at:at + w], seen.at[:, HALF + at:HALF + at + w], ssent, sr, other)

    e = HEAD ** -0.5 * LOG2E

    def attend(early, late):
        def scores(h, chips):
            return _dot(qv[h], jnp.concatenate([kv[2 * c + i, :HEAD, :] for c in chips for i in (0, 1)], 1))

        def values(chips):
            return jnp.concatenate([jnp.concatenate([kv[2 * c + i, HEAD:HEAD + OWN, :], kv[2 * c + i, HEAD + OWN:, :]], 1)
                                    for c in chips for i in (0, 1)], 0)

        def spread(t):
            return jnp.broadcast_to(t, (PAIR, 128))

        def finish(h, s, chips, first):
            s = [s[:, i:i + 128] for i in range(0, s.shape[1], 128)]
            if first:
                row = lax.broadcasted_iota(jnp.int32, (PAIR, 128), 0)
                col = lax.broadcasted_iota(jnp.int32, (PAIR, 128), 1)
                s[-2:] = [jnp.where(row >= col, s[-2], -1e30), jnp.where(row >= col + 128, s[-1], -1e30)]
            at = slice(h * HEAD, (h + 1) * HEAD)
            top = spread(functools.reduce(jnp.maximum, s).max(-1, keepdims=True) * e)
            if not first:
                before = stat[0, h]
                top = jnp.maximum(top, before)
                keep = jnp.exp2(before - top)
            p = [jnp.exp2(t * e - top) for t in s]
            total = spread(functools.reduce(jnp.add, p).sum(-1, keepdims=True))
            o = _dot(jnp.concatenate(p, 1).astype(jnp.bfloat16), values(chips))
            if not first:
                total += stat[1, h] * keep
                o += y[:, at] * jnp.concatenate([keep, keep], 1)
            if first and late:
                stat[0, h] = top
                stat[1, h] = total
                y[:, at] = o
                return
            share = 1 / total
            seen[:, at] = (o * jnp.concatenate([share, share], 1)).astype(jnp.bfloat16)
            if (h + 1) % (8 // SG) == 0:
                w = HALF // SG
                scopy(h // (8 // SG) * w, w).start()

        def heads(chips, first):
            s = scores(0, chips)
            for h in range(8):
                ahead = scores(h + 1, chips) if h < 7 else None
                finish(h, s, chips, first)
                s = ahead
                if first and h in AFTER[:len(late)]:
                    with scope("late_forward"):
                        forward(late[AFTER.index(h)])

        with scope("early_wait"):
            for c in early[:-1]:
                arrived(c, False)
        with scope("early"):
            heads(early, True)
        if late:
            with scope("late_wait"):
                for c in late:
                    arrived(c, False)
            with scope("late"):
                heads(late, False)

    for c in range(CHIPS):
        @pl.when(chip == c)
        def _():
            attend(EARLY[c] + (c,), LATE[c])

    def ycopy(at, w):
        cols = pl.ds(pl.multiple_of(core * HALF + at, w), w)
        return remote(ysend.at[:, at:at + w], out.at[:, cols], ysent, yr, other)

    with scope("o_wait"):
        for c in co:
            c.wait()
    with scope("o_first"):
        for n in range(NO):
            y[:, n * OW:(n + 1) * OW] = _dot(seen[:, :HALF], wov[n, :HALF, :])
    with scope("seen_wait"):
        scopy(0, HALF).wait_recv()

    def second(n, rows, x):
        cols = pl.ds(pl.multiple_of(core * HALF + n * OW, OW), OW)
        t = y[rows, n * OW:(n + 1) * OW] + _dot(seen[rows, HALF:], wov[n, HALF:, :])
        return (t + x[:, cols].astype(jnp.float32)).astype(jnp.bfloat16)

    for n in range(NO):
        with scope("o_theirs"):
            ysend[:, n * OW:(n + 1) * OW] = second(n, theirs, xp)
        ycopy(n * OW, OW).start()
    with scope("o_mine"):
        for n in range(NO):
            out[:, pl.ds(pl.multiple_of(core * HALF + n * OW, OW), OW)] = second(n, mine, xo)

    with scope("y_wait"):
        ycopy(0, HALF).wait()
    with scope("end_wait"):
        xcopy().wait_send()
        scopy(0, HALF).wait_send()
        for c in range(CHIPS):
            @pl.when(chip == c)
            def _():
                count = 1 + sum(frm == c for frm, _ in FIRST + SECOND + THIRD) + len(EARLY[c] + LATE[c])
                remote(kv.at[:count], kv.at[:count], ksent, kr.at[0], other).wait_send()


def _tables():
    half = HEAD // 2
    rate = np.float32(THETA) ** (-np.arange(half, dtype=np.float32) / np.float32(half))
    angle = np.arange(1024, dtype=np.float32)[:, None] * rate.astype(np.float32)
    return np.concatenate([np.cos(angle), np.sin(angle)], 1).astype(np.float32)


def solution(mesh):
    def step(x, gain, wq, wk, wv, wo):
        bf, dma = jnp.bfloat16, pltpu.SemaphoreType.DMA
        return pl.pallas_call(
            _kernel,
            out_shape=pltpu.VMEM((OWN, D), bf),
            in_specs=[pl.BlockSpec(memory_space=pl.ANY)] * 7,
            out_specs=pl.BlockSpec(memory_space=pltpu.VMEM),
            scratch_shapes=[
                pltpu.VMEM((OWN, D), bf), pltpu.VMEM((OWN, D), bf),
                pltpu.VMEM((D,), bf),
                pltpu.VMEM((PAIR, 2 * 128), jnp.float32),
                pltpu.VMEM((PAIR, D), bf),
                pltpu.VMEM((D, 2 * HEAD), bf),
                pltpu.VMEM((NQ, D, QW), bf),
                pltpu.VMEM((NO, D, OW), bf),
                pltpu.VMEM((8, 2 * HEAD, OWN), bf),
                pltpu.VMEM((8, PAIR, HEAD), bf),
                pltpu.VMEM((PAIR, D), bf),
                pltpu.VMEM((PAIR, HALF), jnp.float32),
                pltpu.VMEM((2, 8, PAIR, 128), jnp.float32),
                pltpu.VMEM((OWN, HALF), bf),
                pltpu.SemaphoreType.REGULAR((CHIPS,)),
                dma((5,)), dma((NQ,)), dma, dma((8,)), dma, dma, dma, dma, dma, dma,
            ],
            compiler_params=pltpu.CompilerParams(collective_id=0, has_side_effects=True, vmem_limit_bytes=VMEM),
        )(x, gain, wq, wk, wv, wo, jnp.asarray(_tables()))

    tokens, whole = P(("dp", "sp"), None), P(None, None)
    return jax.shard_map(
        step,
        mesh=mesh,
        in_specs=(tokens, P(None), whole, whole, whole, whole),
        out_specs=tokens,
        check_vma=False,
    )
```

```python
import functools

import jax
import jax.numpy as jnp
import numpy as np
from jax import lax
from jax.experimental import pallas as pl
from jax.experimental.pallas import tpu as pltpu
from jax.sharding import PartitionSpec as P

HEAD = 256
THETA = 10000
LOG2E = 1.4426950408889634
VMEM = 60 * 2**20
MESH = pl.DeviceIdType.MESH
OWN = 128
PAIR = 256
D = 4096
HALF = D // 2
CHIPS = 4
NQ = 4
NO = 2
QW, OW = HALF // NQ, HALF // NO
FIRST = (0, 2), (1, 3), (2, 3), (0, 1)
SECOND = (1, 2),
THIRD = (0, 3),
EARLY = (), (0,), (0,), (1, 2)
LATE = (), (), (1,), (0,)
XF = 64
AFTER = 0, 0, 4, 2


def _dot(a, b):
    return jnp.dot(a, b, preferred_element_type=jnp.float32)


def _kernel(x_hbm, gain_hbm, wq_hbm, wk_hbm, wv_hbm, wo_hbm, turn_hbm, out,
            xo, xp, gv, cs, a, wkv, wqv, wov, kv, qv, seen, y, stat, ysend, ready,
            lsem, qsem, xr, kr, sr, yr, xsent, ksent, ssent, ysent):
    me = lax.axis_index("sp")
    core = lax.rem(me, 2)
    chip = lax.div(me, 2)
    other = me + 1 - 2 * core
    mine = pl.ds(pl.multiple_of(core * OWN, OWN), OWN)
    theirs = pl.ds(pl.multiple_of(OWN - core * OWN, OWN), OWN)
    scope = jax.named_scope

    def alone(f):
        pl.when(chip < CHIPS)(f)

    def fetch(src, dst, sem):
        c = pltpu.make_async_copy(src, dst, sem)
        c.start()
        return c

    def qfetch(n):
        return fetch(wq_hbm.at[:, pl.ds(pl.multiple_of(core * HALF + n * QW, QW), QW)], wqv.at[n], qsem.at[n])

    def ofetch(n):
        cols = pl.ds(pl.multiple_of(core * HALF + n * OW, OW), OW)
        fetch(wo_hbm.at[pl.ds(pl.multiple_of(core * HALF, HALF), HALF), cols], wov.at[n, :HALF, :], qsem.at[n])
        fetch(wo_hbm.at[pl.ds(pl.multiple_of(HALF - core * HALF, HALF), HALF), cols], wov.at[n, HALF:, :], qsem.at[n])
        return pltpu.make_async_copy(wo_hbm.at[:, cols], wov.at[n], qsem.at[n])

    cx = fetch(x_hbm, xo, lsem.at[0])
    cg = fetch(gain_hbm, gv, lsem.at[1])
    barrier = pltpu.get_barrier_semaphore()
    pl.semaphore_signal(barrier, inc=1, device_id={"sp": other}, device_id_type=MESH)
    for c in range(1, CHIPS):
        @pl.when(chip < c)
        def _():
            pl.semaphore_signal(barrier, inc=1, device_id={"sp": c * 2 + core}, device_id_type=MESH)
    rows = pl.ds(pl.multiple_of(chip * PAIR, PAIR), PAIR)
    ck = [fetch(turn_hbm.at[rows, :], cs, lsem.at[2]), fetch(wk_hbm, wkv.at[:, :HEAD], lsem.at[3])]
    cv = fetch(wv_hbm, wkv.at[:, HEAD:], lsem.at[4])
    with scope("barrier"):
        pl.semaphore_wait(barrier, 1 + chip)
    for c in range(CHIPS - 1):
        @pl.when(chip > c)
        def _():
            pl.semaphore_signal(ready.at[chip], inc=1, device_id={"sp": c * 2 + core}, device_id_type=MESH)

    def remote(src, dst, send, recv, to):
        return pltpu.make_async_remote_copy(src_ref=src, dst_ref=dst, send_sem=send, recv_sem=recv, device_id={"sp": to}, device_id_type=MESH)

    def xcopy(src=xo, at=slice(None)):
        return remote(src.at[at, :], xp.at[at, :], xsent, xr, other)

    xcopy(x_hbm, slice(XF, OWN)).start()

    with scope("x_wait"):
        cx.wait()
        cg.wait()
    cq = [qfetch(n) for n in range(NQ)]
    xcopy(xo, slice(0, XF)).start()

    def norm(src, start):
        for i in range(OWN // 16):
            at = pl.ds(pl.multiple_of(start + i * 16, 16), 16)
            wide = src[i * 16:(i + 1) * 16, :].astype(jnp.float32)
            scale = lax.rsqrt(jnp.mean(wide * wide, -1, keepdims=True) + 1e-6)
            a[at, :] = (wide * scale * gv[...].astype(jnp.float32).reshape(1, D)).astype(jnp.bfloat16)

    def turn(t, table):
        cos, sin = table[:, :128], table[:, 128:]
        t = t.astype(jnp.bfloat16).astype(jnp.float32)
        p, q = t[:, :128], t[:, 128:]
        return jnp.concatenate([p * cos - q * sin, q * cos + p * sin], -1).astype(jnp.bfloat16)

    with scope("norm_own"):
        norm(xo, core * OWN)
    def kcopy(i, to, part=slice(None)):
        return remote(kv.at[i, part, :], kv.at[i, part, :], ksent, kr.at[i], to)

    def send(pairs, part, wait=False):
        for c, to in pairs:
            @pl.when(chip == c)
            def _():
                if wait:
                    pl.semaphore_wait(ready.at[to], 1)
                kcopy(me, to * 2 + core, part).start()

    keys, values = slice(0, HEAD), slice(HEAD, 2 * HEAD)
    with scope("k_wait"):
        for c in ck:
            c.wait()
    with scope("k_proj"):
        @alone
        def _():
            kv[me, :HEAD, :] = turn(_dot(a[mine, :], wkv[:, :HEAD]), cs[mine, :]).T
    kcopy(me, other, keys).start()
    with scope("ready"):
        send([(c, to) for c, to in FIRST if c], keys, True)
    with scope("v_proj"):
        cv.wait()

        @alone
        def _():
            v = _dot(a[mine, :], wkv[:, HEAD:]).astype(jnp.bfloat16)
            kv[me, HEAD:HEAD + OWN, :] = v[:, :128]
            kv[me, HEAD + OWN:, :] = v[:, 128:]
    kcopy(me, other, values).start()
    send([(c, to) for c, to in FIRST if c], values)
    send([(c, to) for c, to in FIRST if not c], slice(None), True)

    def arrived(c, mine):
        kcopy(c * 2 + (core if mine else 1 - core), other).wait_recv()

    def forward(c):
        arrived(c, True)
        kcopy(c * 2 + core, other).start()

    with scope("xother_wait"):
        xcopy().wait_recv()
    with scope("norm_other"):
        @alone
        def _():
            norm(xp, OWN - core * OWN)
    with scope("q_wait"):
        cq[0].wait()

    def queries(n):
        t = _dot(a[...], wqv[n])
        for i in range(QW // HEAD):
            qv[n * (QW // HEAD) + i] = turn(t[:, i * HEAD:(i + 1) * HEAD], cs[...])

    with scope("q0"):
        queries(0)
    co = [ofetch(0)]
    send(SECOND, slice(None), True)
    for n in range(1, NQ):
        with scope("q_wait"):
            cq[n].wait()
        with scope("q_proj"):
            queries(n)
        if n == 1:
            co.append(ofetch(1))
        if n == 1:
            send(THIRD, slice(None), True)
        if n == 1:
            with scope("forward"):
                for c in range(1, CHIPS):
                    @pl.when(chip == c)
                    def _():
                        for i in EARLY[c]:
                            forward(i)

    kcopy(other, other).wait_recv()

    def scopy(at, w):
        return remote(seen.at[:, at:at + w], seen.at[:, HALF + at:HALF + at + w], ssent, sr, other)

    e = HEAD ** -0.5 * LOG2E

    def attend(early, late):
        def scores(h, chips):
            return _dot(qv[h], jnp.concatenate([kv[2 * c + i, :HEAD, :] for c in chips for i in (0, 1)], 1))

        def values(chips):
            return jnp.concatenate([jnp.concatenate([kv[2 * c + i, HEAD:HEAD + OWN, :], kv[2 * c + i, HEAD + OWN:, :]], 1)
                                    for c in chips for i in (0, 1)], 0)

        def spread(t):
            return jnp.broadcast_to(t, (PAIR, 128))

        def finish(h, s, chips, first):
            s = [s[:, i:i + 128] for i in range(0, s.shape[1], 128)]
            if first:
                row = lax.broadcasted_iota(jnp.int32, (PAIR, 128), 0)
                col = lax.broadcasted_iota(jnp.int32, (PAIR, 128), 1)
                s[-2:] = [jnp.where(row >= col, s[-2], -1e30), jnp.where(row >= col + 128, s[-1], -1e30)]
            at = slice(h * HEAD, (h + 1) * HEAD)
            top = spread(functools.reduce(jnp.maximum, s).max(-1, keepdims=True) * e)
            if not first:
                before = stat[0, h]
                top = jnp.maximum(top, before)
                keep = jnp.exp2(before - top)
            p = [jnp.exp2(t * e - top) for t in s]
            total = spread(functools.reduce(jnp.add, p).sum(-1, keepdims=True))
            o = _dot(jnp.concatenate(p, 1).astype(jnp.bfloat16), values(chips))
            if not first:
                total += stat[1, h] * keep
                o += y[:, at] * jnp.concatenate([keep, keep], 1)
            if first and late:
                stat[0, h] = top
                stat[1, h] = total
                y[:, at] = o
                return
            share = 1 / total
            seen[:, at] = (o * jnp.concatenate([share, share], 1)).astype(jnp.bfloat16)

        def heads(chips, first, which):
            @alone
            def _():
                s = scores(which[0], chips)
                for h in which:
                    ahead = scores(h + 1, chips) if h + 1 in which else None
                    finish(h, s, chips, first)
                    s = ahead

        with scope("early_wait"):
            for c in early[:-1]:
                arrived(c, False)
        if not late:
            with scope("early"):
                heads(early, True, range(8))
        else:
            after = AFTER[early[-1]]
            if after:
                with scope("early"):
                    heads(early, True, range(after))
            with scope("late_forward"):
                forward(late[0])
            with scope("early"):
                heads(early, True, range(after, 8))
            with scope("late_wait"):
                arrived(late[0], False)
            with scope("late"):
                heads(late, False, range(8))
        with scope("s_start"):
            scopy(0, HALF).start()

    for c in range(CHIPS):
        @pl.when(chip == c)
        def _():
            attend(EARLY[c] + (c,), LATE[c])

    def ycopy(at, w):
        cols = pl.ds(pl.multiple_of(core * HALF + at, w), w)
        return remote(ysend.at[:, at:at + w], out.at[:, cols], ysent, yr, other)

    with scope("o_wait"):
        for c in co:
            c.wait()
    with scope("o_first"):
        @alone
        def _():
            for n in range(NO):
                y[:, n * OW:(n + 1) * OW] = _dot(seen[:, :HALF], wov[n, :HALF, :])
    with scope("seen_wait"):
        scopy(0, HALF).wait_recv()

    def second(n, rows, x):
        cols = pl.ds(pl.multiple_of(core * HALF + n * OW, OW), OW)
        t = y[rows, n * OW:(n + 1) * OW] + _dot(seen[rows, HALF:], wov[n, HALF:, :])
        return (t + x[:, cols].astype(jnp.float32)).astype(jnp.bfloat16)

    for n in range(NO):
        with scope("o_theirs"):
            ysend[:, n * OW:(n + 1) * OW] = second(n, theirs, xp)
        ycopy(n * OW, OW).start()
    with scope("o_mine"):
        for n in range(NO):
            out[:, pl.ds(pl.multiple_of(core * HALF + n * OW, OW), OW)] = second(n, mine, xo)

    with scope("y_wait"):
        ycopy(0, HALF).wait()
    with scope("end_wait"):
        xcopy().wait_send()
        scopy(0, HALF).wait_send()
        for c in range(CHIPS):
            @pl.when(chip == c)
            def _():
                count = 1 + sum(frm == c for frm, _ in FIRST + SECOND + THIRD) + len(EARLY[c] + LATE[c])
                remote(kv.at[:count], kv.at[:count], ksent, kr.at[0], other).wait_send()


def _tables():
    half = HEAD // 2
    rate = np.float32(THETA) ** (-np.arange(half, dtype=np.float32) / np.float32(half))
    angle = np.arange(1024, dtype=np.float32)[:, None] * rate.astype(np.float32)
    return np.concatenate([np.cos(angle), np.sin(angle)], 1).astype(np.float32)


def solution(mesh):
    def step(x, gain, wq, wk, wv, wo):
        bf, dma = jnp.bfloat16, pltpu.SemaphoreType.DMA
        return pl.pallas_call(
            _kernel,
            out_shape=pltpu.VMEM((OWN, D), bf),
            in_specs=[pl.BlockSpec(memory_space=pl.ANY)] * 7,
            out_specs=pl.BlockSpec(memory_space=pltpu.VMEM),
            scratch_shapes=[
                pltpu.VMEM((OWN, D), bf), pltpu.VMEM((OWN, D), bf),
                pltpu.VMEM((D,), bf),
                pltpu.VMEM((PAIR, 2 * 128), jnp.float32),
                pltpu.VMEM((PAIR, D), bf),
                pltpu.VMEM((D, 2 * HEAD), bf),
                pltpu.VMEM((NQ, D, QW), bf),
                pltpu.VMEM((NO, D, OW), bf),
                pltpu.VMEM((8, 2 * HEAD, OWN), bf),
                pltpu.VMEM((8, PAIR, HEAD), bf),
                pltpu.VMEM((PAIR, D), bf),
                pltpu.VMEM((PAIR, HALF), jnp.float32),
                pltpu.VMEM((2, 8, PAIR, 128), jnp.float32),
                pltpu.VMEM((OWN, HALF), bf),
                pltpu.SemaphoreType.REGULAR((CHIPS,)),
                dma((5,)), dma((NQ,)), dma, dma((8,)), dma, dma, dma, dma, dma, dma,
            ],
            compiler_params=pltpu.CompilerParams(collective_id=0, has_side_effects=True, vmem_limit_bytes=VMEM),
        )(x, gain, wq, wk, wv, wo, jnp.asarray(_tables()))

    tokens, whole = P(("dp", "sp"), None), P(None, None)
    return jax.shard_map(
        step,
        mesh=mesh,
        in_specs=(tokens, P(None), whole, whole, whole, whole),
        out_specs=tokens,
        check_vma=False,
    )
```

```python
import functools

import jax
import jax.numpy as jnp
import numpy as np
from jax import lax
from jax.experimental import pallas as pl
from jax.experimental.pallas import tpu as pltpu
from jax.sharding import PartitionSpec as P

HEAD = 256
THETA = 10000
LOG2E = 1.4426950408889634
VMEM = 60 * 2**20
MESH = pl.DeviceIdType.MESH
OWN = 128
PAIR = 256
D = 4096
HALF = D // 2
CHIPS = 4
NQ = 4
NO = 2
QW, OW = HALF // NQ, HALF // NO
FIRST = (0, 2), (1, 3), (2, 3), (0, 1)
SECOND = (1, 2),
THIRD = (0, 3),
EARLY = (), (0,), (0,), (1, 2)
LATE = (), (), (1,), (0,)
XF = 64
AFTER = 0, 0, 4, 4


def _dot(a, b):
    return jnp.dot(a, b, preferred_element_type=jnp.float32)


def _kernel(x_hbm, gain_hbm, wq_hbm, wk_hbm, wv_hbm, wo_hbm, turn_hbm, out,
            xo, xp, gv, cs, a, wkv, wqv, wov, kv, qv, seen, y, stat, ysend, ready,
            lsem, qsem, xr, kr, sr, yr, xsent, ksent, ssent, ysent):
    me = lax.axis_index("sp")
    core = lax.rem(me, 2)
    chip = lax.div(me, 2)
    other = me + 1 - 2 * core
    mine = pl.ds(pl.multiple_of(core * OWN, OWN), OWN)
    theirs = pl.ds(pl.multiple_of(OWN - core * OWN, OWN), OWN)
    scope = jax.named_scope

    def alone(f):
        pl.when(chip < CHIPS)(f)

    def fetch(src, dst, sem):
        c = pltpu.make_async_copy(src, dst, sem)
        c.start()
        return c

    def qfetch(n):
        return fetch(wq_hbm.at[:, pl.ds(pl.multiple_of(core * HALF + n * QW, QW), QW)], wqv.at[n], qsem.at[n])

    def ofetch(n):
        cols = pl.ds(pl.multiple_of(core * HALF + n * OW, OW), OW)
        fetch(wo_hbm.at[pl.ds(pl.multiple_of(core * HALF, HALF), HALF), cols], wov.at[n, :HALF, :], qsem.at[n])
        fetch(wo_hbm.at[pl.ds(pl.multiple_of(HALF - core * HALF, HALF), HALF), cols], wov.at[n, HALF:, :], qsem.at[n])
        return pltpu.make_async_copy(wo_hbm.at[:, cols], wov.at[n], qsem.at[n])

    cx = fetch(x_hbm, xo, lsem.at[0])
    cg = fetch(gain_hbm, gv, lsem.at[1])
    barrier = pltpu.get_barrier_semaphore()
    pl.semaphore_signal(barrier, inc=1, device_id={"sp": other}, device_id_type=MESH)
    for c in range(1, CHIPS):
        @pl.when(chip < c)
        def _():
            pl.semaphore_signal(barrier, inc=1, device_id={"sp": c * 2 + core}, device_id_type=MESH)
    rows = pl.ds(pl.multiple_of(chip * PAIR, PAIR), PAIR)
    ck = [fetch(turn_hbm.at[rows, :], cs, lsem.at[2]), fetch(wk_hbm, wkv.at[:, :HEAD], lsem.at[3])]
    cv = fetch(wv_hbm, wkv.at[:, HEAD:], lsem.at[4])
    with scope("barrier"):
        pl.semaphore_wait(barrier, 1 + chip)
    for c in range(CHIPS - 1):
        @pl.when(chip > c)
        def _():
            pl.semaphore_signal(ready.at[chip], inc=1, device_id={"sp": c * 2 + core}, device_id_type=MESH)

    def remote(src, dst, send, recv, to):
        return pltpu.make_async_remote_copy(src_ref=src, dst_ref=dst, send_sem=send, recv_sem=recv, device_id={"sp": to}, device_id_type=MESH)

    def xcopy(src=xo, at=slice(None)):
        return remote(src.at[at, :], xp.at[at, :], xsent, xr, other)

    xcopy(x_hbm, slice(XF, OWN)).start()

    with scope("x_wait"):
        cx.wait()
        cg.wait()
    cq = [qfetch(n) for n in range(NQ)]
    xcopy(xo, slice(0, XF)).start()

    def norm(src, start):
        for i in range(OWN // 16):
            at = pl.ds(pl.multiple_of(start + i * 16, 16), 16)
            wide = src[i * 16:(i + 1) * 16, :].astype(jnp.float32)
            scale = lax.rsqrt(jnp.mean(wide * wide, -1, keepdims=True) + 1e-6)
            a[at, :] = (wide * scale * gv[...].astype(jnp.float32).reshape(1, D)).astype(jnp.bfloat16)

    def turn(t, table):
        cos, sin = table[:, :128], table[:, 128:]
        t = t.astype(jnp.bfloat16).astype(jnp.float32)
        p, q = t[:, :128], t[:, 128:]
        return jnp.concatenate([p * cos - q * sin, q * cos + p * sin], -1).astype(jnp.bfloat16)

    with scope("norm_own"):
        norm(xo, core * OWN)
    def kcopy(i, to, part=slice(None)):
        return remote(kv.at[i, part, :], kv.at[i, part, :], ksent, kr.at[i], to)

    def send(pairs, part, wait=False):
        for c, to in pairs:
            @pl.when(chip == c)
            def _():
                if wait:
                    pl.semaphore_wait(ready.at[to], 1)
                kcopy(me, to * 2 + core, part).start()

    keys, values = slice(0, HEAD), slice(HEAD, 2 * HEAD)
    with scope("k_wait"):
        for c in ck:
            c.wait()
    with scope("k_proj"):
        @alone
        def _():
            kv[me, :HEAD, :] = turn(_dot(a[mine, :], wkv[:, :HEAD]), cs[mine, :]).T
    kcopy(me, other, keys).start()
    with scope("ready"):
        send([(c, to) for c, to in FIRST if c], keys, True)
    with scope("v_proj"):
        cv.wait()

        @alone
        def _():
            v = _dot(a[mine, :], wkv[:, HEAD:]).astype(jnp.bfloat16)
            kv[me, HEAD:HEAD + OWN, :] = v[:, :128]
            kv[me, HEAD + OWN:, :] = v[:, 128:]
    kcopy(me, other, values).start()
    send([(c, to) for c, to in FIRST if c], values)
    send([(c, to) for c, to in FIRST if not c], slice(None), True)

    def arrived(c, mine):
        kcopy(c * 2 + (core if mine else 1 - core), other).wait_recv()

    def forward(c):
        arrived(c, True)
        kcopy(c * 2 + core, other).start()

    with scope("xother_wait"):
        xcopy().wait_recv()
    with scope("norm_other"):
        @alone
        def _():
            norm(xp, OWN - core * OWN)
    with scope("q_wait"):
        cq[0].wait()

    def queries(n):
        t = _dot(a[...], wqv[n])
        for i in range(QW // HEAD):
            qv[n * (QW // HEAD) + i] = turn(t[:, i * HEAD:(i + 1) * HEAD], cs[...])

    with scope("q0"):
        queries(0)
    co = [ofetch(0)]
    send(SECOND, slice(None), True)
    for n in range(1, NQ):
        with scope("q_wait"):
            cq[n].wait()
        with scope("q_proj"):
            queries(n)
        if n == 1:
            co.append(ofetch(1))
        if n == 1:
            send(THIRD, slice(None), True)
        if n == 1:
            with scope("forward"):
                for c in range(1, CHIPS):
                    @pl.when(chip == c)
                    def _():
                        for i in EARLY[c]:
                            forward(i)

    kcopy(other, other).wait_recv()

    def scopy(at, w):
        return remote(seen.at[:, at:at + w], seen.at[:, HALF + at:HALF + at + w], ssent, sr, other)

    e = HEAD ** -0.5 * LOG2E

    def attend(early, late):
        def scores(h, chips):
            return _dot(qv[h], jnp.concatenate([kv[2 * c + i, :HEAD, :] for c in chips for i in (0, 1)], 1))

        def values(chips):
            return jnp.concatenate([jnp.concatenate([kv[2 * c + i, HEAD:HEAD + OWN, :], kv[2 * c + i, HEAD + OWN:, :]], 1)
                                    for c in chips for i in (0, 1)], 0)

        def spread(t):
            return jnp.broadcast_to(t, (PAIR, 128))

        def finish(h, s, chips, first):
            s = [s[:, i:i + 128] for i in range(0, s.shape[1], 128)]
            if first:
                row = lax.broadcasted_iota(jnp.int32, (PAIR, 128), 0)
                col = lax.broadcasted_iota(jnp.int32, (PAIR, 128), 1)
                s[-2:] = [jnp.where(row >= col, s[-2], -1e30), jnp.where(row >= col + 128, s[-1], -1e30)]
            at = slice(h * HEAD, (h + 1) * HEAD)
            top = spread(functools.reduce(jnp.maximum, s).max(-1, keepdims=True) * e)
            if not first:
                before = stat[0, h]
                top = jnp.maximum(top, before)
                keep = jnp.exp2(before - top)
            p = [jnp.exp2(t * e - top) for t in s]
            total = spread(functools.reduce(jnp.add, p).sum(-1, keepdims=True))
            o = _dot(jnp.concatenate(p, 1).astype(jnp.bfloat16), values(chips))
            if not first:
                total += stat[1, h] * keep
                o += y[:, at] * jnp.concatenate([keep, keep], 1)
            if first and late:
                stat[0, h] = top
                stat[1, h] = total
                y[:, at] = o
                return
            share = 1 / total
            seen[:, at] = (o * jnp.concatenate([share, share], 1)).astype(jnp.bfloat16)

        def heads(chips, first, which):
            @alone
            def _():
                s = scores(which[0], chips)
                for h in which:
                    ahead = scores(h + 1, chips) if h + 1 in which else None
                    finish(h, s, chips, first)
                    s = ahead

        with scope("early_wait"):
            for c in early[:-1]:
                arrived(c, False)
        if not late:
            with scope("early"):
                heads(early, True, range(8))
        else:
            after = AFTER[early[-1]]
            if after:
                with scope("early"):
                    heads(early, True, range(after))
            with scope("late_forward"):
                forward(late[0])
            with scope("early"):
                heads(early, True, range(after, 8))
            with scope("late_wait"):
                arrived(late[0], False)
            with scope("late"):
                heads(late, False, range(8))
        with scope("s_start"):
            scopy(0, HALF).start()

    for c in range(CHIPS):
        @pl.when(chip == c)
        def _():
            attend(EARLY[c] + (c,), LATE[c])

    def ycopy(at, w):
        cols = pl.ds(pl.multiple_of(core * HALF + at, w), w)
        return remote(ysend.at[:, at:at + w], out.at[:, cols], ysent, yr, other)

    with scope("o_wait"):
        for c in co:
            c.wait()
    with scope("o_first"):
        @alone
        def _():
            for n in range(NO):
                y[:, n * OW:(n + 1) * OW] = _dot(seen[:, :HALF], wov[n, :HALF, :])
    with scope("seen_wait"):
        scopy(0, HALF).wait_recv()

    def second(n, rows, x):
        cols = pl.ds(pl.multiple_of(core * HALF + n * OW, OW), OW)
        t = y[rows, n * OW:(n + 1) * OW] + _dot(seen[rows, HALF:], wov[n, HALF:, :])
        return (t + x[:, cols].astype(jnp.float32)).astype(jnp.bfloat16)

    for n in range(NO):
        with scope("o_theirs"):
            ysend[:, n * OW:(n + 1) * OW] = second(n, theirs, xp)
        ycopy(n * OW, OW).start()
    with scope("o_mine"):
        for n in range(NO):
            out[:, pl.ds(pl.multiple_of(core * HALF + n * OW, OW), OW)] = second(n, mine, xo)

    with scope("y_wait"):
        ycopy(0, HALF).wait()
    with scope("end_wait"):
        xcopy().wait_send()
        scopy(0, HALF).wait_send()
        for c in range(CHIPS):
            @pl.when(chip == c)
            def _():
                count = 1 + sum(frm == c for frm, _ in FIRST + SECOND + THIRD) + len(EARLY[c] + LATE[c])
                remote(kv.at[:count], kv.at[:count], ksent, kr.at[0], other).wait_send()


def _tables():
    half = HEAD // 2
    rate = np.float32(THETA) ** (-np.arange(half, dtype=np.float32) / np.float32(half))
    angle = np.arange(1024, dtype=np.float32)[:, None] * rate.astype(np.float32)
    return np.concatenate([np.cos(angle), np.sin(angle)], 1).astype(np.float32)


def solution(mesh):
    def step(x, gain, wq, wk, wv, wo):
        bf, dma = jnp.bfloat16, pltpu.SemaphoreType.DMA
        return pl.pallas_call(
            _kernel,
            out_shape=pltpu.VMEM((OWN, D), bf),
            in_specs=[pl.BlockSpec(memory_space=pl.ANY)] * 7,
            out_specs=pl.BlockSpec(memory_space=pltpu.VMEM),
            scratch_shapes=[
                pltpu.VMEM((OWN, D), bf), pltpu.VMEM((OWN, D), bf),
                pltpu.VMEM((D,), bf),
                pltpu.VMEM((PAIR, 2 * 128), jnp.float32),
                pltpu.VMEM((PAIR, D), bf),
                pltpu.VMEM((D, 2 * HEAD), bf),
                pltpu.VMEM((NQ, D, QW), bf),
                pltpu.VMEM((NO, D, OW), bf),
                pltpu.VMEM((8, 2 * HEAD, OWN), bf),
                pltpu.VMEM((8, PAIR, HEAD), bf),
                pltpu.VMEM((PAIR, D), bf),
                pltpu.VMEM((PAIR, HALF), jnp.float32),
                pltpu.VMEM((2, 8, PAIR, 128), jnp.float32),
                pltpu.VMEM((OWN, HALF), bf),
                pltpu.SemaphoreType.REGULAR((CHIPS,)),
                dma((5,)), dma((NQ,)), dma, dma((8,)), dma, dma, dma, dma, dma, dma,
            ],
            compiler_params=pltpu.CompilerParams(collective_id=0, has_side_effects=True, vmem_limit_bytes=VMEM),
        )(x, gain, wq, wk, wv, wo, jnp.asarray(_tables()))

    tokens, whole = P(("dp", "sp"), None), P(None, None)
    return jax.shard_map(
        step,
        mesh=mesh,
        in_specs=(tokens, P(None), whole, whole, whole, whole),
        out_specs=tokens,
        check_vma=False,
    )
```

```python
import functools

import jax
import jax.numpy as jnp
import numpy as np
from jax import lax
from jax.experimental import pallas as pl
from jax.experimental.pallas import tpu as pltpu
from jax.sharding import PartitionSpec as P

HEAD = 256
THETA = 10000
LOG2E = 1.4426950408889634
VMEM = 60 * 2**20
MESH = pl.DeviceIdType.MESH
OWN = 128
PAIR = 256
D = 4096
HALF = D // 2
CHIPS = 4
NQ = 4
NO = 2
QW, OW = HALF // NQ, HALF // NO
FIRST = (0, 2), (1, 3), (2, 3), (0, 1)
SECOND = (1, 2),
THIRD = (0, 3),
EARLY = (), (0,), (0,), (1, 2)
LATE = (), (), (1,), (0,)
XF = 64
AFTER = 0, 0, 4, 4


def _dot(a, b):
    return jnp.dot(a, b, preferred_element_type=jnp.float32)


def _kernel(x_hbm, gain_hbm, wq_hbm, wk_hbm, wv_hbm, wo_hbm, turn_hbm, out,
            xo, xp, gv, cs, a, wkv, wqv, wov, kv, qv, seen, y, stat, ysend, ready,
            lsem, qsem, xr, kr, sr, yr, xsent, ksent, ssent, ysent):
    me = lax.axis_index("sp")
    core = lax.rem(me, 2)
    chip = lax.div(me, 2)
    other = me + 1 - 2 * core
    mine = pl.ds(pl.multiple_of(core * OWN, OWN), OWN)
    theirs = pl.ds(pl.multiple_of(OWN - core * OWN, OWN), OWN)
    scope = jax.named_scope

    def alone(f):
        pl.when(chip < CHIPS)(f)

    def fetch(src, dst, sem):
        c = pltpu.make_async_copy(src, dst, sem)
        c.start()
        return c

    def qfetch(n):
        return fetch(wq_hbm.at[:, pl.ds(pl.multiple_of(core * HALF + n * QW, QW), QW)], wqv.at[n], qsem.at[n])

    def ofetch(n):
        cols = pl.ds(pl.multiple_of(core * HALF + n * OW, OW), OW)
        fetch(wo_hbm.at[pl.ds(pl.multiple_of(core * HALF, HALF), HALF), cols], wov.at[n, :HALF, :], qsem.at[n])
        fetch(wo_hbm.at[pl.ds(pl.multiple_of(HALF - core * HALF, HALF), HALF), cols], wov.at[n, HALF:, :], qsem.at[n])
        return pltpu.make_async_copy(wo_hbm.at[:, cols], wov.at[n], qsem.at[n])

    cx = fetch(x_hbm, xo, lsem.at[0])
    cg = fetch(gain_hbm, gv, lsem.at[1])
    barrier = pltpu.get_barrier_semaphore()
    pl.semaphore_signal(barrier, inc=1, device_id={"sp": other}, device_id_type=MESH)
    for c in range(1, CHIPS):
        @pl.when(chip < c)
        def _():
            pl.semaphore_signal(barrier, inc=1, device_id={"sp": c * 2 + core}, device_id_type=MESH)
    rows = pl.ds(pl.multiple_of(chip * PAIR, PAIR), PAIR)
    ck = [fetch(turn_hbm.at[rows, :], cs, lsem.at[2]), fetch(wk_hbm, wkv.at[:, :HEAD], lsem.at[3])]
    cv = fetch(wv_hbm, wkv.at[:, HEAD:], lsem.at[4])
    with scope("barrier"):
        pl.semaphore_wait(barrier, 1 + chip)
    for c in range(CHIPS - 1):
        @pl.when(chip > c)
        def _():
            pl.semaphore_signal(ready.at[chip], inc=1, device_id={"sp": c * 2 + core}, device_id_type=MESH)

    def remote(src, dst, send, recv, to):
        return pltpu.make_async_remote_copy(src_ref=src, dst_ref=dst, send_sem=send, recv_sem=recv, device_id={"sp": to}, device_id_type=MESH)

    def xcopy(src=xo, at=slice(None)):
        return remote(src.at[at, :], xp.at[at, :], xsent, xr, other)

    xcopy(x_hbm, slice(XF, OWN)).start()

    with scope("x_wait"):
        cx.wait()
        cg.wait()
    cq = [qfetch(n) for n in range(NQ)]
    xcopy(xo, slice(0, XF)).start()

    def norm(src, start):
        for i in range(OWN // 16):
            at = pl.ds(pl.multiple_of(start + i * 16, 16), 16)
            wide = src[i * 16:(i + 1) * 16, :].astype(jnp.float32)
            scale = lax.rsqrt(jnp.mean(wide * wide, -1, keepdims=True) + 1e-6)
            a[at, :] = (wide * scale * gv[...].astype(jnp.float32).reshape(1, D)).astype(jnp.bfloat16)

    def turn(t, table):
        cos, sin = table[:, :128], table[:, 128:]
        t = t.astype(jnp.bfloat16).astype(jnp.float32)
        p, q = t[:, :128], t[:, 128:]
        return jnp.concatenate([p * cos - q * sin, q * cos + p * sin], -1).astype(jnp.bfloat16)

    with scope("norm_own"):
        norm(xo, core * OWN)
    def kcopy(i, to, part=slice(None)):
        return remote(kv.at[i, part, :], kv.at[i, part, :], ksent, kr.at[i], to)

    def send(pairs, part, wait=False):
        for c, to in pairs:
            @pl.when(chip == c)
            def _():
                if wait:
                    pl.semaphore_wait(ready.at[to], 1)
                kcopy(me, to * 2 + core, part).start()

    keys, values = slice(0, HEAD), slice(HEAD, 2 * HEAD)
    with scope("k_wait"):
        for c in ck:
            c.wait()
    with scope("k_proj"):
        @alone
        def _():
            kv[me, :HEAD, :] = turn(_dot(a[mine, :], wkv[:, :HEAD]), cs[mine, :]).T
    kcopy(me, other, keys).start()
    with scope("ready"):
        send([(c, to) for c, to in FIRST if c], keys, True)
    with scope("v_proj"):
        cv.wait()

        @alone
        def _():
            v = _dot(a[mine, :], wkv[:, HEAD:]).astype(jnp.bfloat16)
            kv[me, HEAD:HEAD + OWN, :] = v[:, :128]
            kv[me, HEAD + OWN:, :] = v[:, 128:]
    kcopy(me, other, values).start()
    send([(c, to) for c, to in FIRST if c], values)
    send([(c, to) for c, to in FIRST if not c], slice(None), True)

    def arrived(c, mine):
        kcopy(c * 2 + (core if mine else 1 - core), other).wait_recv()

    def forward(c):
        arrived(c, True)
        kcopy(c * 2 + core, other).start()

    with scope("xother_wait"):
        xcopy().wait_recv()
    with scope("norm_other"):
        @alone
        def _():
            norm(xp, OWN - core * OWN)
    with scope("q_wait"):
        cq[0].wait()

    def queries(n):
        t = _dot(a[...], wqv[n])
        for i in range(QW // HEAD):
            qv[n * (QW // HEAD) + i] = turn(t[:, i * HEAD:(i + 1) * HEAD], cs[...])

    with scope("q0"):
        queries(0)
    co = [ofetch(0)]
    send(SECOND, slice(None), True)
    for n in range(1, NQ):
        with scope("q_wait"):
            cq[n].wait()
        with scope("q_proj"):
            queries(n)
        if n == 1:
            co.append(ofetch(1))
        if n == 1:
            send(THIRD, slice(None), True)
        if n == 1:
            with scope("forward"):
                for c in range(1, CHIPS):
                    @pl.when(chip == c)
                    def _():
                        for i in EARLY[c]:
                            forward(i)

    kcopy(other, other).wait_recv()

    def scopy(at, w):
        return remote(seen.at[:, at:at + w], seen.at[:, HALF + at:HALF + at + w], ssent, sr, other)

    e = HEAD ** -0.5 * LOG2E

    def attend(early, late):
        def scores(h, chips):
            return _dot(qv[h], jnp.concatenate([kv[2 * c + i, :HEAD, :] for c in chips for i in (0, 1)], 1))

        def values(chips):
            return jnp.concatenate([jnp.concatenate([kv[2 * c + i, HEAD:HEAD + OWN, :], kv[2 * c + i, HEAD + OWN:, :]], 1)
                                    for c in chips for i in (0, 1)], 0)

        def spread(t):
            return jnp.broadcast_to(t, (PAIR, 128))

        def finish(h, s, chips, first):
            s = [s[:, i:i + 128] for i in range(0, s.shape[1], 128)]
            if first:
                row = lax.broadcasted_iota(jnp.int32, (PAIR, 128), 0)
                col = lax.broadcasted_iota(jnp.int32, (PAIR, 128), 1)
                s[-2:] = [jnp.where(row >= col, s[-2], -1e30), jnp.where(row >= col + 128, s[-1], -1e30)]
            at = slice(h * HEAD, (h + 1) * HEAD)
            top = spread(functools.reduce(jnp.maximum, s).max(-1, keepdims=True) * e)
            if not first:
                before = stat[0, h]
                top = jnp.maximum(top, before)
                keep = jnp.exp2(before - top)
            p = [jnp.exp2(t * e - top) for t in s]
            total = spread(functools.reduce(jnp.add, p).sum(-1, keepdims=True))
            o = _dot(jnp.concatenate(p, 1).astype(jnp.bfloat16), values(chips))
            if not first:
                total += stat[1, h] * keep
                o += y[:, at] * jnp.concatenate([keep, keep], 1)
            if first and late:
                stat[0, h] = top
                stat[1, h] = total
                y[:, at] = o
                return
            share = 1 / total
            seen[:, at] = (o * jnp.concatenate([share, share], 1)).astype(jnp.bfloat16)

        def heads(chips, first, which):
            @alone
            def _():
                s = scores(which[0], chips)
                for h in which:
                    ahead = scores(h + 1, chips) if h + 1 in which else None
                    finish(h, s, chips, first)
                    s = ahead

        with scope("early_wait"):
            for c in early[:-1]:
                arrived(c, False)
        if not late:
            with scope("early"):
                heads(early, True, range(8))
        else:
            after = AFTER[early[-1]]
            if after:
                with scope("early"):
                    heads(early, True, range(after))
            with scope("late_forward"):
                forward(late[0])
            with scope("early"):
                heads(early, True, range(after, 8))
            with scope("late_wait"):
                arrived(late[0], False)
            with scope("late"):
                heads(late, False, range(8))
        with scope("s_start"):
            scopy(0, HALF).start()

    for c in range(CHIPS):
        @pl.when(chip == c)
        def _():
            attend(EARLY[c] + (c,), LATE[c])

    def ycopy(at, w):
        cols = pl.ds(pl.multiple_of(core * HALF + at, w), w)
        return remote(ysend.at[:, at:at + w], out.at[:, cols], ysent, yr, other)

    with scope("o_wait"):
        for c in co:
            c.wait()
    with scope("o_first"):
        for n in range(NO):
            y[:, n * OW:(n + 1) * OW] = _dot(seen[:, :HALF], wov[n, :HALF, :])
    with scope("seen_wait"):
        scopy(0, HALF).wait_recv()

    def second(n, rows, x):
        cols = pl.ds(pl.multiple_of(core * HALF + n * OW, OW), OW)
        t = y[rows, n * OW:(n + 1) * OW] + _dot(seen[rows, HALF:], wov[n, HALF:, :])
        return (t + x[:, cols].astype(jnp.float32)).astype(jnp.bfloat16)

    for n in range(NO):
        with scope("o_theirs"):
            ysend[:, n * OW:(n + 1) * OW] = second(n, theirs, xp)
        ycopy(n * OW, OW).start()
    with scope("o_mine"):
        for n in range(NO):
            out[:, pl.ds(pl.multiple_of(core * HALF + n * OW, OW), OW)] = second(n, mine, xo)

    with scope("y_wait"):
        ycopy(0, HALF).wait()
    with scope("end_wait"):
        xcopy().wait_send()
        scopy(0, HALF).wait_send()
        for c in range(CHIPS):
            @pl.when(chip == c)
            def _():
                count = 1 + sum(frm == c for frm, _ in FIRST + SECOND + THIRD) + len(EARLY[c] + LATE[c])
                remote(kv.at[:count], kv.at[:count], ksent, kr.at[0], other).wait_send()


def _tables():
    half = HEAD // 2
    rate = np.float32(THETA) ** (-np.arange(half, dtype=np.float32) / np.float32(half))
    angle = np.arange(1024, dtype=np.float32)[:, None] * rate.astype(np.float32)
    return np.concatenate([np.cos(angle), np.sin(angle)], 1).astype(np.float32)


def solution(mesh):
    def step(x, gain, wq, wk, wv, wo):
        bf, dma = jnp.bfloat16, pltpu.SemaphoreType.DMA
        return pl.pallas_call(
            _kernel,
            out_shape=pltpu.VMEM((OWN, D), bf),
            in_specs=[pl.BlockSpec(memory_space=pl.ANY)] * 7,
            out_specs=pl.BlockSpec(memory_space=pltpu.VMEM),
            scratch_shapes=[
                pltpu.VMEM((OWN, D), bf), pltpu.VMEM((OWN, D), bf),
                pltpu.VMEM((D,), bf),
                pltpu.VMEM((PAIR, 2 * 128), jnp.float32),
                pltpu.VMEM((PAIR, D), bf),
                pltpu.VMEM((D, 2 * HEAD), bf),
                pltpu.VMEM((NQ, D, QW), bf),
                pltpu.VMEM((NO, D, OW), bf),
                pltpu.VMEM((8, 2 * HEAD, OWN), bf),
                pltpu.VMEM((8, PAIR, HEAD), bf),
                pltpu.VMEM((PAIR, D), bf),
                pltpu.VMEM((PAIR, HALF), jnp.float32),
                pltpu.VMEM((2, 8, PAIR, 128), jnp.float32),
                pltpu.VMEM((OWN, HALF), bf),
                pltpu.SemaphoreType.REGULAR((CHIPS,)),
                dma((5,)), dma((NQ,)), dma, dma((8,)), dma, dma, dma, dma, dma, dma,
            ],
            compiler_params=pltpu.CompilerParams(collective_id=0, has_side_effects=True, vmem_limit_bytes=VMEM),
        )(x, gain, wq, wk, wv, wo, jnp.asarray(_tables()))

    tokens, whole = P(("dp", "sp"), None), P(None, None)
    return jax.shard_map(
        step,
        mesh=mesh,
        in_specs=(tokens, P(None), whole, whole, whole, whole),
        out_specs=tokens,
        check_vma=False,
    )
```
